256 devices in a mesh: fsdp: 32 (over z, y), tp: 4 (over x), job: 2 (over core).
Axes of the slice: x: 4, y: 4, z: 8, core: 2. Of those that a mesh axis runs over, the one named last changes fastest.
Arguments:
- slopes_in: float32 [1024, 128, 1024], P('job', 'fsdp', 'tp'), parts along dimension 0, may hold values from -6 to 6
- moments_in: float32 [1024, 128, 1024], P('job', 'fsdp', 'tp'), parts along dimension 0, may hold values from -6 to 6
- weights_in: float32 [1024, 128, 1024], P('job', 'fsdp', 'tp'), parts along dimension 0, may hold values from -0.1875 to 0.1875
Outputs:
- new_weights: float32 [1024, 128, 1024], P('job', 'fsdp', 'tp'), parts along dimension 0
- new_momentum: float32 [1024, 128, 1024], P('job', 'fsdp', 'tp'), parts along dimension 0
The draws below stay inside these ranges and needn't reach their ends.
There are 2 independent parts, one for each index of `job`. The reference program is written for one: setup_inputs(seed, part) draws one part's arguments, and reference() takes and returns one part's arrays. A program takes and returns all parts, laid end to end along the dimension named above; each array names one. Nothing has to cross between parts.
All inputs are finite; a program needn't handle non-finite values.
Results may differ from the reference program's by a relative error of at most 0.00019.
Values sent between devices are 32-bit elements; how exact they have to be, the bound alone decides.
A program may use at most 128 MiB of HBM per device.

```python
import jax
import jax.numpy as jnp
from jax import lax

SIDE = 128
WIDE = 1024
MATS = 512
ITERS = 5


def steps_of(stream_key, dims, shards, smallest, largest):
    def one(dim, parts):
        heights = jax.random.uniform(jax.random.fold_in(jax.random.fold_in(stream_key, 6), dim), (parts,), jnp.float32, smallest / len(shards), largest / len(shards))
        return jnp.repeat(jnp.exp(heights), dims[dim] // parts).reshape((-1,) + (1,) * (len(dims) - dim - 1))

    factor_of = one(*shards[0])
    for cut in shards[1:]:
        factor_of = factor_of * one(*cut)
    return factor_of


def scatter_about(own_key, extent, scale, bound, pieces=(), kind=jnp.bfloat16):
    drawn = jax.random.normal(own_key, extent, jnp.float32) * scale
    if len(pieces) > 0:
        drawn = steps_of(own_key, extent, pieces, -0.22, 0.18) * drawn
    return jnp.clip(drawn, min=-bound, max=bound).astype(kind)


def setup_inputs(seed: int = 0, part: int = 0) -> dict:
    arg_keys = jax.random.split(jax.random.key(seed), 4)
    part_splits = jax.random.split(jax.random.fold_in(arg_keys[3], part), 4)
    return {
        "slopes_in": scatter_about(part_splits[0], (MATS, SIDE, WIDE), 1.0, 6.0, ((1, 32), (2, 4)), jnp.float32),
        "moments_in": scatter_about(part_splits[1], (MATS, SIDE, WIDE), 1.0, 6.0, ((1, 32), (2, 4)), jnp.float32),
        "weights_in": scatter_about(part_splits[2], (MATS, SIDE, WIDE), 0.03, 0.1875, ((1, 32), (2, 4)), jnp.float32),
    }


hold_rate = 0.9
learn_rate = 0.8

def reference(slopes_in, moments_in, weights_in):
    new_momentum = hold_rate * moments_in + slopes_in

    def orthogonal_one(stack):
        iterate = stack[None]
        iterate = iterate * lax.rsqrt(lax.optimization_barrier(jnp.sum(iterate * iterate, axis=(1, 2), keepdims=True)) + 1e-06)
        for step in range(ITERS):
            gram = jnp.einsum('mik,mjk->mij', iterate, iterate, precision=lax.Precision.HIGHEST)
            mixed = -4.775 * gram + 2.0315 * jnp.einsum('mij,mjk->mik', gram, gram, precision=lax.Precision.HIGHEST)
            iterate = 3.4445 * iterate + jnp.einsum('mij,mjk->mik', mixed, iterate, precision=lax.Precision.HIGHEST)
        return iterate[0]
    iterate = lax.map(orthogonal_one, new_momentum)
    new_weights = weights_in - learn_rate * iterate
    return (new_weights, new_momentum)
```

```python
import functools

import jax
import jax.numpy as jnp
from jax import lax
from jax.experimental import pallas as pl
from jax.experimental.pallas import tpu as pltpu
from jax.sharding import PartitionSpec as P

ITERS = 5
NZ = 8
NY = 4
NX = 4
NP = NY * NX
CHUNKS = 4

hold_rate = 0.9
learn_rate = 0.8

MESH = pl.DeviceIdType.MESH
HIGHEST = lax.Precision.HIGHEST


def dot_nn(a, b):
    return lax.dot_general(a, b, (((1,), (0,)), ((), ())), precision=HIGHEST, preferred_element_type=jnp.float32)


def dot_nt(a, b):
    return lax.dot_general(a, b, (((1,), (1,)), ((), ())), precision=HIGHEST, preferred_element_type=jnp.float32)


def kernel(
    mom, out, zin, xyin, res, xyout, xs,
    zi_send, zi_recv, pi_send, pi_recv, po_send, po_recv, zo_send, zo_recv,
):
    f, x, j = lax.axis_index("fsdp"), lax.axis_index("tp"), lax.axis_index("job")
    z, y = f // NY, lax.rem(f, NY)
    own = y * NX + x

    def along_z(d):
        return (lax.rem(z + d, NZ) * NY + y, x, j)

    def in_plane(dy, dx):
        return (z * NY + lax.rem(y + dy, NY), lax.rem(x + dx, NX), j)

    steps_z = (1, 7, 2, 6, 3, 5, 4)
    steps_p = [(dy, dx) for dx in (1, 3, 0, 2) for dy in (1, 3, 0, 2) if (dy, dx) != (0, 0)]

    barrier = pltpu.get_barrier_semaphore()
    for d in steps_z:
        pl.semaphore_signal(barrier, inc=1, device_id=along_z(d), device_id_type=MESH)
    for dy, dx in steps_p:
        pl.semaphore_signal(barrier, inc=1, device_id=in_plane(dy, dx), device_id_type=MESH)
    pl.semaphore_wait(barrier, len(steps_z) + len(steps_p))

    def send(src, dst, send_sem, recv_sem, device):
        pltpu.make_async_remote_copy(
            src_ref=src, dst_ref=dst, send_sem=send_sem, recv_sem=recv_sem, device_id=device, device_id_type=MESH
        ).start()

    def wait(ref, sem):
        pltpu.make_async_copy(ref, ref, sem).wait()

    for c in range(CHUNKS):
        for d in steps_z:
            to = lax.rem(z + d, NZ)
            send(mom.at[c, to], zin.at[c, d], zi_send.at[c], zi_recv.at[c], along_z(d))
    for c in range(CHUNKS):
        zin[c, 0] = mom[c, z]

    def plane_in(c):
        wait(zin.at[c, pl.ds(1, NZ - 1)], zi_recv.at[c])
        for dy, dx in steps_p:
            to = lax.rem(y + dy, NY) * NX + lax.rem(x + dx, NX)
            send(zin.at[c, :, to], xyin.at[c, dx * NY + dy], pi_send.at[c], pi_recv.at[c], in_plane(dy, dx))
        xyin[c, 0] = zin[c, :, own]

    def work(c):
        wait(xyin.at[c, pl.ds(1, NP - 1)], pi_recv.at[c])
        for k in range(NX):
            xs[:, k * 256 : (k + 1) * 256] = xyin[c, k * NY : (k + 1) * NY].reshape(128, 256)
        total = jnp.sum(xs[...] * xs[...])
        xs[...] = xs[...] * lax.rsqrt(jnp.full((1, 1), total, jnp.float32) + 1e-06)

        def step(_, carry):
            gram = dot_nt(xs[...], xs[...])
            mixed = -4.775 * gram + 2.0315 * dot_nn(gram, gram)
            for k in range(NX):
                part = xs[:, k * 256 : (k + 1) * 256]
                xs[:, k * 256 : (k + 1) * 256] = 3.4445 * part + dot_nn(mixed, part)
            return carry

        lax.fori_loop(0, ITERS, step, 0)
        for k in range(NX):
            res[c, k * NY : (k + 1) * NY] = xs[:, k * 256 : (k + 1) * 256].reshape(NY, NZ, 4, 256)
        xyout[c, :, own] = res[c, 0]
        for dy, dx in steps_p:
            back = in_plane(NY - dy, NX - dx)
            send(res.at[c, dx * NY + dy], xyout.at[c, :, own], po_send.at[c], po_recv.at[c], back)

    def z_out(c):
        wait(res.at[c, pl.ds(1, NP - 1)], po_recv.at[c])
        for d in steps_z:
            send(xyout.at[c, d], out.at[c, z], zo_send.at[c], zo_recv.at[c], along_z(NZ - d))
        out[c, z] = xyout[c, 0]

    def step(s, carry):
        @pl.when(s < CHUNKS)
        def _():
            plane_in(s)

        @pl.when(jnp.logical_and(s >= 1, s <= CHUNKS))
        def _():
            work(s - 1)

        @pl.when(s >= 2)
        def _():
            z_out(s - 2)

        return carry

    lax.fori_loop(0, CHUNKS + 2, step, 0)
    for c in range(CHUNKS):
        wait(zin.at[c, pl.ds(1, NZ - 1)], zo_recv.at[c])
        wait(zin.at[c, pl.ds(1, NZ - 1)], zi_send.at[c])
        wait(zin.at[c, pl.ds(1, NZ - 1)], zo_send.at[c])
        wait(xyin.at[c, pl.ds(1, NP - 1)], pi_send.at[c])
        wait(xyin.at[c, pl.ds(1, NP - 1)], po_send.at[c])


def exchange(mom):
    block = (4, 256)
    return pl.pallas_call(
        kernel,
        name="exchange",
        out_shape=jax.ShapeDtypeStruct((CHUNKS, NZ, NP, *block), jnp.float32),
        in_specs=[pl.BlockSpec(memory_space=pltpu.VMEM)],
        out_specs=pl.BlockSpec(memory_space=pltpu.VMEM),
        scratch_shapes=[
            pltpu.VMEM((CHUNKS, NZ, NP, *block), jnp.float32),
            pltpu.VMEM((CHUNKS, NP, NZ, *block), jnp.float32),
            pltpu.VMEM((CHUNKS, NP, NZ, *block), jnp.float32),
            pltpu.VMEM((CHUNKS, NZ, NP, *block), jnp.float32),
            pltpu.VMEM((128, 1024), jnp.float32),
        ]
        + [pltpu.SemaphoreType.DMA((CHUNKS,))] * 8,
        compiler_params=pltpu.CompilerParams(collective_id=0, has_side_effects=True, vmem_limit_bytes=32 * 2**20),
    )(mom)


def body(slopes_in, moments_in, weights_in):
    new_momentum = hold_rate * moments_in + slopes_in
    back = exchange(new_momentum.reshape(CHUNKS, NZ, NP, 4, 256)).reshape(slopes_in.shape)
    new_weights = weights_in - learn_rate * back
    return (new_weights, new_momentum)


def solution(mesh):
    placed = (P("job", "fsdp", "tp"), P("job", "fsdp", "tp"), P("job", "fsdp", "tp"))
    return jax.shard_map(
        body,
        mesh=mesh,
        in_specs=placed,
        out_specs=(P("job", "fsdp", "tp"), P("job", "fsdp", "tp")),
        check_vma=False,
    )
```

```python
import functools

import jax
import jax.numpy as jnp
from jax import lax
from jax.experimental import pallas as pl
from jax.experimental.pallas import tpu as pltpu
from jax.sharding import PartitionSpec as P

ITERS = 5
NZ = 8
NY = 4
NX = 4
NP = NY * NX
CHUNKS = 4

hold_rate = 0.9
learn_rate = 0.8

MESH = pl.DeviceIdType.MESH
HIGHEST = lax.Precision.HIGHEST


def dot_nn(a, b):
    return lax.dot_general(a, b, (((1,), (0,)), ((), ())), precision=HIGHEST, preferred_element_type=jnp.float32)


def dot_nt(a, b):
    return lax.dot_general(a, b, (((1,), (1,)), ((), ())), precision=HIGHEST, preferred_element_type=jnp.float32)


def kernel(
    slopes, moments, weights, out, mom, slopes_v, moments_v, weights_v, zin, xyin, res, xyout, xs,
    load_s, load_m, load_w, zi_send, zi_recv, pi_send, pi_recv, po_send, po_recv, zo_send, zo_recv,
):
    f, x, j = lax.axis_index("fsdp"), lax.axis_index("tp"), lax.axis_index("job")
    z, y = f // NY, lax.rem(f, NY)
    own = y * NX + x

    def along_z(d):
        return (lax.rem(z + d, NZ) * NY + y, x, j)

    def in_plane(dy, dx):
        return (z * NY + lax.rem(y + dy, NY), lax.rem(x + dx, NX), j)

    steps_z = (1, 7, 2, 6, 3, 5, 4)
    steps_back = (4, 3, 5, 2, 6, 1, 7)
    steps_p = [(dy, dx) for dx in (1, 3, 0, 2) for dy in (1, 3, 0, 2) if (dy, dx) != (0, 0)]

    loads = []
    for c in range(CHUNKS):
        loads.append(pltpu.make_async_copy(slopes.at[c], slopes_v.at[c], load_s.at[c]))
        loads.append(pltpu.make_async_copy(moments.at[c], moments_v.at[c], load_m.at[c]))
    load_weights = pltpu.make_async_copy(weights, weights_v, load_w)
    for copy in loads:
        copy.start()
    barrier = pltpu.get_barrier_semaphore()
    for d in steps_z:
        pl.semaphore_signal(barrier, inc=1, device_id=along_z(d), device_id_type=MESH)
    for dy, dx in steps_p:
        pl.semaphore_signal(barrier, inc=1, device_id=in_plane(dy, dx), device_id_type=MESH)
    def send(src, dst, send_sem, recv_sem, device):
        pltpu.make_async_remote_copy(
            src_ref=src, dst_ref=dst, send_sem=send_sem, recv_sem=recv_sem, device_id=device, device_id_type=MESH
        ).start()

    def wait(ref, sem):
        pltpu.make_async_copy(ref, ref, sem).wait()

    for c in range(CHUNKS):
        loads[2 * c].wait()
        loads[2 * c + 1].wait()
        mom[c] = hold_rate * moments_v[c] + slopes_v[c]
        if c == 0:
            pl.semaphore_wait(barrier, len(steps_z) + len(steps_p))
        for d in steps_z:
            to = lax.rem(z + d, NZ)
            send(mom.at[c, to], zin.at[c, d], zi_send.at[c], zi_recv.at[c], along_z(d))
    load_weights.start()
    for c in range(CHUNKS):
        zin[c, 0] = mom[c, z]

    def plane_in(c):
        wait(zin.at[c, pl.ds(1, NZ - 1)], zi_recv.at[c])
        for dy, dx in steps_p:
            to = lax.rem(y + dy, NY) * NX + lax.rem(x + dx, NX)
            send(zin.at[c, :, to], xyin.at[c, dx * NY + dy], pi_send.at[c], pi_recv.at[c], in_plane(dy, dx))
        xyin[c, 0] = zin[c, :, own]

    def work(c):
        wait(xyin.at[c, pl.ds(1, NP - 1)], pi_recv.at[c])
        for k in range(NX):
            xs[:, k * 256 : (k + 1) * 256] = xyin[c, k * NY : (k + 1) * NY].reshape(128, 256)
        total = jnp.sum(xs[...] * xs[...])
        xs[...] = xs[...] * lax.rsqrt(jnp.full((1, 1), total, jnp.float32) + 1e-06)

        def step(_, carry):
            gram = dot_nt(xs[...], xs[...])
            mixed = -4.775 * gram + 2.0315 * dot_nn(gram, gram)
            for k in range(NX):
                part = xs[:, k * 256 : (k + 1) * 256]
                xs[:, k * 256 : (k + 1) * 256] = 3.4445 * part + dot_nn(mixed, part)
            return carry

        lax.fori_loop(0, ITERS, step, 0)
        for k in range(NX):
            res[c, k * NY : (k + 1) * NY] = (learn_rate * xs[:, k * 256 : (k + 1) * 256]).reshape(NY, NZ, 4, 256)
        xyout[c, :, own] = res[c, 0]
        for dy, dx in steps_p:
            back = in_plane(NY - dy, NX - dx)
            send(res.at[c, dx * NY + dy], xyout.at[c, :, own], po_send.at[c], po_recv.at[c], back)

    def z_out(c):
        wait(res.at[c, pl.ds(1, NP - 1)], po_recv.at[c])
        for d in steps_back:
            send(xyout.at[c, d], out.at[c, z], zo_send.at[c], zo_recv.at[c], along_z(NZ - d))
        out[c, z] = xyout[c, 0]

    def step(s, carry):
        @pl.when(s < CHUNKS)
        def _():
            plane_in(s)

        @pl.when(jnp.logical_and(s >= 1, s <= CHUNKS))
        def _():
            work(s - 1)

        @pl.when(s >= 2)
        def _():
            z_out(s - 2)

        return carry

    lax.fori_loop(0, CHUNKS + 2, step, 0)
    load_weights.wait()
    for c in range(CHUNKS):
        wait(zin.at[c, pl.ds(1, NZ - 1)], zo_recv.at[c])
        out[c] = weights_v[c] - out[c]
    for c in range(CHUNKS):
        wait(zin.at[c, pl.ds(1, NZ - 1)], zi_send.at[c])
        wait(zin.at[c, pl.ds(1, NZ - 1)], zo_send.at[c])
        wait(xyin.at[c, pl.ds(1, NP - 1)], pi_send.at[c])
        wait(xyin.at[c, pl.ds(1, NP - 1)], po_send.at[c])


def put_out(new_weights_v, new_momentum_v, new_weights, new_momentum, sems):
    pairs = ((new_weights_v, new_weights), (new_momentum_v, new_momentum))
    copies = [
        pltpu.make_async_copy(src.at[c], dst.at[c], sems.at[i, c])
        for c in range(CHUNKS) for i, (src, dst) in enumerate(pairs)
    ]
    for copy in copies:
        copy.start()
    for copy in copies:
        copy.wait()


def exchange(slopes, moments, weights):
    shape = (CHUNKS, NZ, NP, 4, 256)
    whole = jax.ShapeDtypeStruct(shape, jnp.float32)
    split = pltpu.VMEM(shape, jnp.float32)
    plane = pltpu.VMEM((CHUNKS, NP, NZ, 4, 256), jnp.float32)
    new_weights, new_momentum = pl.pallas_call(
        kernel,
        name="exchange",
        out_shape=(whole, whole),
        in_specs=[pl.BlockSpec(memory_space=pltpu.HBM)] * 3,
        out_specs=[pl.BlockSpec(memory_space=pltpu.VMEM)] * 2,
        scratch_shapes=[split, split, split, split, plane, plane, split, pltpu.VMEM((128, 1024), jnp.float32)]
        + [pltpu.SemaphoreType.DMA((CHUNKS,))] * 2
        + [pltpu.SemaphoreType.DMA]
        + [pltpu.SemaphoreType.DMA((CHUNKS,))] * 8,
        compiler_params=pltpu.CompilerParams(collective_id=0, has_side_effects=True, vmem_limit_bytes=40 * 2**20),
    )(*[pltpu.with_memory_space_constraint(a.reshape(shape), pltpu.HBM) for a in (slopes, moments, weights)])
    new_weights, new_momentum = pl.pallas_call(
        put_out,
        name="put_out",
        out_shape=(whole, whole),
        in_specs=[pl.BlockSpec(memory_space=pltpu.VMEM)] * 2,
        out_specs=[pl.BlockSpec(memory_space=pltpu.HBM)] * 2,
        scratch_shapes=[pltpu.SemaphoreType.DMA((2, CHUNKS))],
        compiler_params=pltpu.CompilerParams(vmem_limit_bytes=8 * 2**20),
    )(new_weights, new_momentum)
    return new_weights.reshape(slopes.shape), new_momentum.reshape(slopes.shape)


def body(slopes_in, moments_in, weights_in):
    return exchange(slopes_in, moments_in, weights_in)


def solution(mesh):
    placed = (P("job", "fsdp", "tp"), P("job", "fsdp", "tp"), P("job", "fsdp", "tp"))
    return jax.shard_map(
        body,
        mesh=mesh,
        in_specs=placed,
        out_specs=(P("job", "fsdp", "tp"), P("job", "fsdp", "tp")),
        check_vma=False,
    )
```

```python
import functools

import jax
import jax.numpy as jnp
from jax import lax
from jax.experimental import pallas as pl
from jax.experimental.pallas import tpu as pltpu
from jax.sharding import PartitionSpec as P

ITERS = 5
NZ = 8
NY = 4
NX = 4
NP = NY * NX
CHUNKS = 4

hold_rate = 0.9
learn_rate = 0.8

MESH = pl.DeviceIdType.MESH


def dot_nn(a, b):
    return lax.dot_general(a, b, (((1,), (0,)), ((), ())), preferred_element_type=jnp.float32)


def dot_nt(a, b):
    return lax.dot_general(a, b, (((1,), (1,)), ((), ())), preferred_element_type=jnp.float32)


def thirds(v):
    high = v.astype(jnp.bfloat16)
    rest = v - high.astype(jnp.float32)
    mid = rest.astype(jnp.bfloat16)
    return high, mid, (rest - mid.astype(jnp.float32)).astype(jnp.bfloat16)


def product(a, b):
    left = jnp.concatenate([a[0], a[1]], axis=1)
    ends = jnp.concatenate([a[0], a[2]], axis=1)
    small = dot_nn(ends, jnp.concatenate([b[2], b[0]], axis=0)) + dot_nn(left, jnp.concatenate([b[1], b[1]], axis=0))
    return small + dot_nn(left, jnp.concatenate([b[0], b[0]], axis=0))


def kernel(
    slopes, moments, weights, out, mom, slopes_v, moments_v, weights_v, zin, xyin, res, xyout, xs, top, low,
    load_s, load_m, load_w, zi_send, zi_recv, pi_send, pi_recv, po_send, po_recv, zo_send, zo_recv,
):
    f, x, j = lax.axis_index("fsdp"), lax.axis_index("tp"), lax.axis_index("job")
    z, y = f // NY, lax.rem(f, NY)
    own = y * NX + x

    def along_z(d):
        return (lax.rem(z + d, NZ) * NY + y, x, j)

    def in_plane(dy, dx):
        return (z * NY + lax.rem(y + dy, NY), lax.rem(x + dx, NX), j)

    steps_z = (1, 7, 2, 6, 3, 5, 4)
    steps_back = (4, 3, 5, 2, 6, 1, 7)
    steps_p = [(dy, dx) for dx in (1, 3, 0, 2) for dy in (1, 3, 0, 2) if (dy, dx) != (0, 0)]

    loads = []
    for c in range(CHUNKS):
        loads.append(pltpu.make_async_copy(slopes.at[c], slopes_v.at[c], load_s.at[c]))
        loads.append(pltpu.make_async_copy(moments.at[c], moments_v.at[c], load_m.at[c]))
    load_weights = pltpu.make_async_copy(weights, weights_v, load_w)
    for copy in loads:
        copy.start()
    barrier = pltpu.get_barrier_semaphore()
    for d in steps_z:
        pl.semaphore_signal(barrier, inc=1, device_id=along_z(d), device_id_type=MESH)
    for dy, dx in steps_p:
        pl.semaphore_signal(barrier, inc=1, device_id=in_plane(dy, dx), device_id_type=MESH)
    def send(src, dst, send_sem, recv_sem, device):
        pltpu.make_async_remote_copy(
            src_ref=src, dst_ref=dst, send_sem=send_sem, recv_sem=recv_sem, device_id=device, device_id_type=MESH
        ).start()

    def wait(ref, sem):
        pltpu.make_async_copy(ref, ref, sem).wait()

    for c in range(CHUNKS):
        loads[2 * c].wait()
        loads[2 * c + 1].wait()
        mom[c] = hold_rate * moments_v[c] + slopes_v[c]
        if c == 0:
            pl.semaphore_wait(barrier, len(steps_z) + len(steps_p))
        for d in steps_z:
            to = lax.rem(z + d, NZ)
            send(mom.at[c, to], zin.at[c, d], zi_send.at[c], zi_recv.at[c], along_z(d))
    load_weights.start()
    for c in range(CHUNKS):
        zin[c, 0] = mom[c, z]

    def plane_in(c):
        wait(zin.at[c, pl.ds(1, NZ - 1)], zi_recv.at[c])
        for dy, dx in steps_p:
            to = lax.rem(y + dy, NY) * NX + lax.rem(x + dx, NX)
            send(zin.at[c, :, to], xyin.at[c, dx * NY + dy], pi_send.at[c], pi_recv.at[c], in_plane(dy, dx))
        xyin[c, 0] = zin[c, :, own]

    def work(c):
        wait(xyin.at[c, pl.ds(1, NP - 1)], pi_recv.at[c])
        for k in range(NX):
            xs[:, k * 256 : (k + 1) * 256] = xyin[c, k * NY : (k + 1) * NY].reshape(128, 256)
        total = jnp.sum(xs[...] * xs[...])
        xs[...] = xs[...] * lax.rsqrt(jnp.full((1, 1), total, jnp.float32) + 1e-06)

        def step(_, carry):
            for k in range(NX):
                at = slice(k * 256, (k + 1) * 256)
                top[0:128, at], top[128:256, at], low[:, at] = thirds(xs[:, at])
            upper = dot_nt(top[0:128], top[...])
            mixed_terms = upper[:, 128:] + dot_nt(top[0:128], low[...])
            gram = upper[:, :128] + (dot_nt(top[128:256], top[128:256]) + mixed_terms + mixed_terms.T)
            parts = thirds(gram)
            mixed = thirds(-4.775 * gram + 2.0315 * product(parts, parts))
            for k in range(NX):
                at = slice(k * 256, (k + 1) * 256)
                xs[:, at] = 3.4445 * xs[:, at] + product(mixed, (top[0:128, at], top[128:256, at], low[:, at]))
            return carry

        lax.fori_loop(0, ITERS, step, 0)
        for k in range(NX):
            res[c, k * NY : (k + 1) * NY] = (learn_rate * xs[:, k * 256 : (k + 1) * 256]).reshape(NY, NZ, 4, 256)
        xyout[c, :, own] = res[c, 0]
        for dy, dx in steps_p:
            back = in_plane(NY - dy, NX - dx)
            send(res.at[c, dx * NY + dy], xyout.at[c, :, own], po_send.at[c], po_recv.at[c], back)

    def z_out(c):
        wait(res.at[c, pl.ds(1, NP - 1)], po_recv.at[c])
        for d in steps_back:
            send(xyout.at[c, d], out.at[c, z], zo_send.at[c], zo_recv.at[c], along_z(NZ - d))
        out[c, z] = xyout[c, 0]

    def step(s, carry):
        @pl.when(s < CHUNKS)
        def _():
            plane_in(s)

        @pl.when(jnp.logical_and(s >= 1, s <= CHUNKS))
        def _():
            work(s - 1)

        @pl.when(s >= 2)
        def _():
            z_out(s - 2)

        return carry

    lax.fori_loop(0, CHUNKS + 2, step, 0)
    load_weights.wait()
    for c in range(CHUNKS):
        wait(zin.at[c, pl.ds(1, NZ - 1)], zo_recv.at[c])
        out[c] = weights_v[c] - out[c]
    for c in range(CHUNKS):
        wait(zin.at[c, pl.ds(1, NZ - 1)], zi_send.at[c])
        wait(zin.at[c, pl.ds(1, NZ - 1)], zo_send.at[c])
        wait(xyin.at[c, pl.ds(1, NP - 1)], pi_send.at[c])
        wait(xyin.at[c, pl.ds(1, NP - 1)], po_send.at[c])


def put_out(new_weights_v, new_momentum_v, new_weights, new_momentum, sems):
    pairs = ((new_weights_v, new_weights), (new_momentum_v, new_momentum))
    copies = [
        pltpu.make_async_copy(src.at[c], dst.at[c], sems.at[i, c])
        for c in range(CHUNKS) for i, (src, dst) in enumerate(pairs)
    ]
    for copy in copies:
        copy.start()
    for copy in copies:
        copy.wait()


def exchange(slopes, moments, weights):
    shape = (CHUNKS, NZ, NP, 4, 256)
    whole = jax.ShapeDtypeStruct(shape, jnp.float32)
    split = pltpu.VMEM(shape, jnp.float32)
    plane = pltpu.VMEM((CHUNKS, NP, NZ, 4, 256), jnp.float32)
    new_weights, new_momentum = pl.pallas_call(
        kernel,
        name="exchange",
        out_shape=(whole, whole),
        in_specs=[pl.BlockSpec(memory_space=pltpu.HBM)] * 3,
        out_specs=[pl.BlockSpec(memory_space=pltpu.VMEM)] * 2,
        scratch_shapes=[split, split, split, split, plane, plane, split, pltpu.VMEM((128, 1024), jnp.float32)]
        + [pltpu.VMEM((256, 1024), jnp.bfloat16), pltpu.VMEM((128, 1024), jnp.bfloat16)]
        + [pltpu.SemaphoreType.DMA((CHUNKS,))] * 2
        + [pltpu.SemaphoreType.DMA]
        + [pltpu.SemaphoreType.DMA((CHUNKS,))] * 8,
        compiler_params=pltpu.CompilerParams(collective_id=0, has_side_effects=True, vmem_limit_bytes=40 * 2**20),
    )(*[pltpu.with_memory_space_constraint(a.reshape(shape), pltpu.HBM) for a in (slopes, moments, weights)])
    new_weights, new_momentum = pl.pallas_call(
        put_out,
        name="put_out",
        out_shape=(whole, whole),
        in_specs=[pl.BlockSpec(memory_space=pltpu.VMEM)] * 2,
        out_specs=[pl.BlockSpec(memory_space=pltpu.HBM)] * 2,
        scratch_shapes=[pltpu.SemaphoreType.DMA((2, CHUNKS))],
        compiler_params=pltpu.CompilerParams(vmem_limit_bytes=8 * 2**20),
    )(new_weights, new_momentum)
    return new_weights.reshape(slopes.shape), new_momentum.reshape(slopes.shape)


def body(slopes_in, moments_in, weights_in):
    return exchange(slopes_in, moments_in, weights_in)


def solution(mesh):
    placed = (P("job", "fsdp", "tp"), P("job", "fsdp", "tp"), P("job", "fsdp", "tp"))
    return jax.shard_map(
        body,
        mesh=mesh,
        in_specs=placed,
        out_specs=(P("job", "fsdp", "tp"), P("job", "fsdp", "tp")),
        check_vma=False,
    )
```

```python
import functools

import jax
import jax.numpy as jnp
from jax import lax
from jax.experimental import pallas as pl
from jax.experimental.pallas import tpu as pltpu
from jax.sharding import PartitionSpec as P

ITERS = 5
NZ = 8
NY = 4
NX = 4
NP = NY * NX
CHUNKS = 4

hold_rate = 0.9
learn_rate = 0.8

MESH = pl.DeviceIdType.MESH


def dot_nn(a, b):
    return lax.dot_general(a, b, (((1,), (0,)), ((), ())), preferred_element_type=jnp.float32)


def dot_nt(a, b):
    return lax.dot_general(a, b, (((1,), (1,)), ((), ())), preferred_element_type=jnp.float32)


def thirds(v):
    high = v.astype(jnp.bfloat16)
    rest = v - high.astype(jnp.float32)
    mid = rest.astype(jnp.bfloat16)
    return high, mid, (rest - mid.astype(jnp.float32)).astype(jnp.bfloat16)


def product(a, b):
    left = jnp.concatenate([a[0], a[1]], axis=1)
    ends = jnp.concatenate([a[0], a[2]], axis=1)
    small = dot_nn(ends, jnp.concatenate([b[2], b[0]], axis=0)) + dot_nn(left, jnp.concatenate([b[1], b[1]], axis=0))
    return small + dot_nn(left, jnp.concatenate([b[0], b[0]], axis=0))


def kernel(
    slopes, moments, weights, out, mom, slopes_v, moments_v, weights_v, zin, xyin, res, xyout, xs, top, low,
    round_sem, load_s, load_m, load_w, zi_send, zi_recv, pi_send, pi_recv, po_send, po_recv, zo_send, zo_recv,
):
    f, x, j = lax.axis_index("fsdp"), lax.axis_index("tp"), lax.axis_index("job")
    z, y = f // NY, lax.rem(f, NY)
    own = y * NX + x

    def along_z(d):
        return (lax.rem(z + d, NZ) * NY + y, x, j)

    def in_plane(dy, dx):
        return (z * NY + lax.rem(y + dy, NY), lax.rem(x + dx, NX), j)

    steps_z = (1, 7, 2, 6, 3, 5, 4)
    steps_back = (4, 3, 5, 2, 6, 1, 7)
    steps_p = [(dy, dx) for dx in (1, 3, 0, 2) for dy in (1, 3, 0, 2) if (dy, dx) != (0, 0)]

    loads = []
    for c in range(CHUNKS):
        loads.append(pltpu.make_async_copy(slopes.at[c], slopes_v.at[c], load_s.at[c]))
        loads.append(pltpu.make_async_copy(moments.at[c], moments_v.at[c], load_m.at[c]))
    load_weights = pltpu.make_async_copy(weights, weights_v, load_w)
    for copy in loads[:2]:
        copy.start()
    barrier = pltpu.get_barrier_semaphore()
    near = [along_z(1), along_z(NZ - 1), in_plane(1, 0), in_plane(NY - 1, 0), in_plane(0, 1), in_plane(0, NX - 1)]
    for device in near:
        pl.semaphore_signal(barrier, inc=1, device_id=device, device_id_type=MESH)

    def tell(k):
        for device in near:
            pl.semaphore_signal(round_sem.at[k], inc=1, device_id=device, device_id_type=MESH)

    def hear(k):
        pl.semaphore_wait(round_sem.at[k], len(near))

    def send(src, dst, send_sem, recv_sem, device):
        pltpu.make_async_remote_copy(
            src_ref=src, dst_ref=dst, send_sem=send_sem, recv_sem=recv_sem, device_id=device, device_id_type=MESH
        ).start()

    def wait(ref, sem):
        pltpu.make_async_copy(ref, ref, sem).wait()

    def send_in(c, d):
        send(mom.at[c, lax.rem(z + d, NZ)], zin.at[c, d], zi_send.at[c], zi_recv.at[c], along_z(d))

    def momentum(c):
        loads[2 * c].wait()
        loads[2 * c + 1].wait()
        mom[c] = hold_rate * moments_v[c] + slopes_v[c]

    pl.semaphore_wait(barrier, len(near))
    tell(0)
    momentum(0)
    for copy in loads[2:]:
        copy.start()
    send_in(0, 1)
    send_in(0, NZ - 1)
    hear(0)
    tell(1)
    send_in(0, 2)
    send_in(0, NZ - 2)
    hear(1)
    tell(2)
    send_in(0, 3)
    send_in(0, NZ - 3)
    for c in range(1, CHUNKS):
        momentum(c)
    hear(2)
    send_in(0, 4)
    for c in range(1, CHUNKS):
        for d in steps_z:
            send_in(c, d)
    load_weights.start()
    for c in range(CHUNKS):
        zin[c, 0] = mom[c, z]

    def plane_in(c):
        wait(zin.at[c, pl.ds(1, NZ - 1)], zi_recv.at[c])
        for dy, dx in steps_p:
            to = lax.rem(y + dy, NY) * NX + lax.rem(x + dx, NX)
            send(zin.at[c, :, to], xyin.at[c, dx * NY + dy], pi_send.at[c], pi_recv.at[c], in_plane(dy, dx))
        xyin[c, 0] = zin[c, :, own]

    def work(c):
        wait(xyin.at[c, pl.ds(1, NP - 1)], pi_recv.at[c])
        for k in range(NX):
            xs[:, k * 256 : (k + 1) * 256] = xyin[c, k * NY : (k + 1) * NY].reshape(128, 256)
        total = jnp.sum(xs[...] * xs[...])
        xs[...] = xs[...] * lax.rsqrt(jnp.full((1, 1), total, jnp.float32) + 1e-06)

        def step(_, carry):
            for k in range(NX):
                at = slice(k * 256, (k + 1) * 256)
                top[0:128, at], top[128:256, at], low[:, at] = thirds(xs[:, at])
            upper = dot_nt(top[0:128], top[...])
            mixed_terms = upper[:, 128:] + dot_nt(top[0:128], low[...])
            gram = upper[:, :128] + (dot_nt(top[128:256], top[128:256]) + mixed_terms + mixed_terms.T)
            parts = thirds(gram)
            mixed = thirds(-4.775 * gram + 2.0315 * product(parts, parts))
            for k in range(NX):
                at = slice(k * 256, (k + 1) * 256)
                xs[:, at] = 3.4445 * xs[:, at] + product(mixed, (top[0:128, at], top[128:256, at], low[:, at]))
            return carry

        lax.fori_loop(0, ITERS, step, 0)
        for k in range(NX):
            res[c, k * NY : (k + 1) * NY] = (learn_rate * xs[:, k * 256 : (k + 1) * 256]).reshape(NY, NZ, 4, 256)
        xyout[c, :, own] = res[c, 0]
        for dy, dx in steps_p:
            back = in_plane(NY - dy, NX - dx)
            send(res.at[c, dx * NY + dy], xyout.at[c, :, own], po_send.at[c], po_recv.at[c], back)

    def z_out(c):
        wait(res.at[c, pl.ds(1, NP - 1)], po_recv.at[c])
        for d in steps_back:
            send(xyout.at[c, d], out.at[c, z], zo_send.at[c], zo_recv.at[c], along_z(NZ - d))
        out[c, z] = xyout[c, 0]

    def step(s, carry):
        @pl.when(s < CHUNKS)
        def _():
            plane_in(s)

        @pl.when(jnp.logical_and(s >= 1, s <= CHUNKS))
        def _():
            work(s - 1)

        @pl.when(s >= 2)
        def _():
            z_out(s - 2)

        return carry

    lax.fori_loop(0, CHUNKS + 2, step, 0)
    load_weights.wait()
    for c in range(CHUNKS):
        wait(zin.at[c, pl.ds(1, NZ - 1)], zo_recv.at[c])
        out[c] = weights_v[c] - out[c]
    for c in range(CHUNKS):
        wait(zin.at[c, pl.ds(1, NZ - 1)], zi_send.at[c])
        wait(zin.at[c, pl.ds(1, NZ - 1)], zo_send.at[c])
        wait(xyin.at[c, pl.ds(1, NP - 1)], pi_send.at[c])
        wait(xyin.at[c, pl.ds(1, NP - 1)], po_send.at[c])


def put_out(new_weights_v, new_momentum_v, new_weights, new_momentum, sems):
    pairs = ((new_weights_v, new_weights), (new_momentum_v, new_momentum))
    copies = [
        pltpu.make_async_copy(src.at[c], dst.at[c], sems.at[i, c])
        for c in range(CHUNKS) for i, (src, dst) in enumerate(pairs)
    ]
    for copy in copies:
        copy.start()
    for copy in copies:
        copy.wait()


def exchange(slopes, moments, weights):
    shape = (CHUNKS, NZ, NP, 4, 256)
    whole = jax.ShapeDtypeStruct(shape, jnp.float32)
    split = pltpu.VMEM(shape, jnp.float32)
    plane = pltpu.VMEM((CHUNKS, NP, NZ, 4, 256), jnp.float32)
    new_weights, new_momentum = pl.pallas_call(
        kernel,
        name="exchange",
        out_shape=(whole, whole),
        in_specs=[pl.BlockSpec(memory_space=pltpu.HBM)] * 3,
        out_specs=[pl.BlockSpec(memory_space=pltpu.VMEM)] * 2,
        scratch_shapes=[split, split, split, split, plane, plane, split, pltpu.VMEM((128, 1024), jnp.float32)]
        + [pltpu.VMEM((256, 1024), jnp.bfloat16), pltpu.VMEM((128, 1024), jnp.bfloat16)]
        + [pltpu.SemaphoreType.REGULAR((3,))]
        + [pltpu.SemaphoreType.DMA((CHUNKS,))] * 2
        + [pltpu.SemaphoreType.DMA]
        + [pltpu.SemaphoreType.DMA((CHUNKS,))] * 8,
        compiler_params=pltpu.CompilerParams(collective_id=0, has_side_effects=True, vmem_limit_bytes=40 * 2**20),
    )(*[pltpu.with_memory_space_constraint(a.reshape(shape), pltpu.HBM) for a in (slopes, moments, weights)])
    new_weights, new_momentum = pl.pallas_call(
        put_out,
        name="put_out",
        out_shape=(whole, whole),
        in_specs=[pl.BlockSpec(memory_space=pltpu.VMEM)] * 2,
        out_specs=[pl.BlockSpec(memory_space=pltpu.HBM)] * 2,
        scratch_shapes=[pltpu.SemaphoreType.DMA((2, CHUNKS))],
        compiler_params=pltpu.CompilerParams(vmem_limit_bytes=8 * 2**20),
    )(new_weights, new_momentum)
    return new_weights.reshape(slopes.shape), new_momentum.reshape(slopes.shape)


def body(slopes_in, moments_in, weights_in):
    return exchange(slopes_in, moments_in, weights_in)


def solution(mesh):
    placed = (P("job", "fsdp", "tp"), P("job", "fsdp", "tp"), P("job", "fsdp", "tp"))
    return jax.shard_map(
        body,
        mesh=mesh,
        in_specs=placed,
        out_specs=(P("job", "fsdp", "tp"), P("job", "fsdp", "tp")),
        check_vma=False,
    )
```

```python
import functools

import jax
import jax.numpy as jnp
from jax import lax
from jax.experimental import pallas as pl
from jax.experimental.pallas import tpu as pltpu
from jax.sharding import PartitionSpec as P

ITERS = 5
NZ = 8
NY = 4
NX = 4
NP = NY * NX
CHUNKS = 4

hold_rate = 0.9
learn_rate = 0.8

MESH = pl.DeviceIdType.MESH


def dot_nn(a, b):
    return lax.dot_general(a, b, (((1,), (0,)), ((), ())), preferred_element_type=jnp.float32)


def dot_nt(a, b):
    return lax.dot_general(a, b, (((1,), (1,)), ((), ())), preferred_element_type=jnp.float32)


def thirds(v):
    high = v.astype(jnp.bfloat16)
    rest = v - high.astype(jnp.float32)
    mid = rest.astype(jnp.bfloat16)
    return high, mid, (rest - mid.astype(jnp.float32)).astype(jnp.bfloat16)


def product(a, b):
    left = jnp.concatenate([a[0], a[1]], axis=1)
    ends = jnp.concatenate([a[0], a[2]], axis=1)
    small = dot_nn(ends, jnp.concatenate([b[2], b[0]], axis=0)) + dot_nn(left, jnp.concatenate([b[1], b[1]], axis=0))
    return small + dot_nn(left, jnp.concatenate([b[0], b[0]], axis=0))


def kernel(
    slopes, moments, weights, out, mom, last_w, slopes_v, moments_v, weights_v, zin, xyin, res, xyout, xs, top, low,
    round_sem, load_s, load_m, load_w, zi_send, zi_recv, pi_send, pi_recv, po_send, po_recv, zo_send, zo_recv,
):
    f, x, j = lax.axis_index("fsdp"), lax.axis_index("tp"), lax.axis_index("job")
    z, y = f // NY, lax.rem(f, NY)
    own = y * NX + x

    def along_z(d):
        return (lax.rem(z + d, NZ) * NY + y, x, j)

    def in_plane(dy, dx):
        return (z * NY + lax.rem(y + dy, NY), lax.rem(x + dx, NX), j)

    steps_z = (1, 7, 2, 6, 3, 5, 4)
    steps_back = (4, 3, 5, 2, 6, 1, 7)
    steps_p = [(dy, dx) for dx in (1, 3, 0, 2) for dy in (1, 3, 0, 2) if (dy, dx) != (0, 0)]

    loads = []
    for c in range(CHUNKS):
        loads.append(pltpu.make_async_copy(slopes.at[c], slopes_v.at[c], load_s.at[c]))
        loads.append(pltpu.make_async_copy(moments.at[c], moments_v.at[c], load_m.at[c]))
    load_weights = pltpu.make_async_copy(weights.at[pl.ds(0, CHUNKS - 1)], weights_v, load_w.at[0])
    load_last = pltpu.make_async_copy(weights.at[CHUNKS - 1], last_w, load_w.at[1])
    for copy in loads[:2]:
        copy.start()
    barrier = pltpu.get_barrier_semaphore()
    near = [along_z(1), along_z(NZ - 1), in_plane(1, 0), in_plane(NY - 1, 0), in_plane(0, 1), in_plane(0, NX - 1)]
    for device in near:
        pl.semaphore_signal(barrier, inc=1, device_id=device, device_id_type=MESH)

    def tell(k):
        for device in near:
            pl.semaphore_signal(round_sem.at[k], inc=1, device_id=device, device_id_type=MESH)

    def hear(k):
        pl.semaphore_wait(round_sem.at[k], len(near))

    def send(src, dst, send_sem, recv_sem, device):
        pltpu.make_async_remote_copy(
            src_ref=src, dst_ref=dst, send_sem=send_sem, recv_sem=recv_sem, device_id=device, device_id_type=MESH
        ).start()

    def wait(ref, sem):
        pltpu.make_async_copy(ref, ref, sem).wait()

    def send_in(c, d):
        send(mom.at[c, lax.rem(z + d, NZ)], zin.at[c, d], zi_send.at[c], zi_recv.at[c], along_z(d))

    def momentum(c):
        loads[2 * c].wait()
        loads[2 * c + 1].wait()
        mom[c] = hold_rate * moments_v[c] + slopes_v[c]

    pl.semaphore_wait(barrier, len(near))
    tell(0)
    momentum(0)
    for copy in loads[2:]:
        copy.start()
    send_in(0, 1)
    send_in(0, NZ - 1)
    hear(0)
    tell(1)
    send_in(0, 2)
    send_in(0, NZ - 2)
    hear(1)
    tell(2)
    send_in(0, 3)
    send_in(0, NZ - 3)
    hear(2)
    send_in(0, 4)
    for c in range(1, CHUNKS):
        momentum(c)
        for d in steps_z:
            send_in(c, d)
    load_weights.start()
    load_last.start()
    for c in range(CHUNKS):
        zin[c, 0] = mom[c, z]

    def plane_in(c):
        wait(zin.at[c, pl.ds(1, NZ - 1)], zi_recv.at[c])
        for dy, dx in steps_p:
            to = lax.rem(y + dy, NY) * NX + lax.rem(x + dx, NX)
            send(zin.at[c, :, to], xyin.at[c, dx * NY + dy], pi_send.at[c], pi_recv.at[c], in_plane(dy, dx))
        xyin[c, 0] = zin[c, :, own]

    def work(c):
        wait(xyin.at[c, pl.ds(1, NP - 1)], pi_recv.at[c])
        for k in range(NX):
            xs[:, k * 256 : (k + 1) * 256] = xyin[c, k * NY : (k + 1) * NY].reshape(128, 256)
        total = jnp.sum(xs[...] * xs[...])
        xs[...] = xs[...] * lax.rsqrt(jnp.full((1, 1), total, jnp.float32) + 1e-06)

        def step(_, carry):
            for k in range(NX):
                at = slice(k * 256, (k + 1) * 256)
                top[0:128, at], top[128:256, at], low[:, at] = thirds(xs[:, at])
            upper = dot_nt(top[0:128], top[...])
            mixed_terms = upper[:, 128:] + dot_nt(top[0:128], low[...])
            gram = upper[:, :128] + (dot_nt(top[128:256], top[128:256]) + mixed_terms + mixed_terms.T)
            parts = thirds(gram)
            mixed = thirds(-4.775 * gram + 2.0315 * product(parts, parts))
            for k in range(NX):
                at = slice(k * 256, (k + 1) * 256)
                xs[:, at] = 3.4445 * xs[:, at] + product(mixed, (top[0:128, at], top[128:256, at], low[:, at]))
            return carry

        lax.fori_loop(0, ITERS, step, 0)
        for k in range(NX):
            res[c, k * NY : (k + 1) * NY] = (learn_rate * xs[:, k * 256 : (k + 1) * 256]).reshape(NY, NZ, 4, 256)
        xyout[c, :, own] = res[c, 0]
        for dy, dx in steps_p:
            back = in_plane(NY - dy, NX - dx)
            send(res.at[c, dx * NY + dy], xyout.at[c, :, own], po_send.at[c], po_recv.at[c], back)

    def z_out(c):
        wait(res.at[c, pl.ds(1, NP - 1)], po_recv.at[c])
        for d in steps_back:
            send(xyout.at[c, d], out.at[c, z], zo_send.at[c], zo_recv.at[c], along_z(NZ - d))
        out[c, z] = xyout[c, 0]

    def step(s, carry):
        @pl.when(s < CHUNKS)
        def _():
            plane_in(s)

        @pl.when(jnp.logical_and(s >= 1, s <= CHUNKS))
        def _():
            work(s - 1)

        @pl.when(s >= 2)
        def _():
            z_out(s - 2)

        return carry

    lax.fori_loop(0, CHUNKS + 2, step, 0)
    load_weights.wait()
    load_last.wait()
    for c in range(CHUNKS):
        wait(zin.at[c, pl.ds(1, NZ - 1)], zo_recv.at[c])
        if c < CHUNKS - 1:
            out[c] = weights_v[c] - out[c]
    for c in range(CHUNKS):
        wait(zin.at[c, pl.ds(1, NZ - 1)], zi_send.at[c])
        wait(zin.at[c, pl.ds(1, NZ - 1)], zo_send.at[c])
        wait(xyin.at[c, pl.ds(1, NP - 1)], pi_send.at[c])
        wait(xyin.at[c, pl.ds(1, NP - 1)], po_send.at[c])


def put_out(new_weights_v, new_momentum_v, last_w, new_weights, new_momentum, last_v, sems):
    final = CHUNKS - 1
    copies = [pltpu.make_async_copy(new_weights_v.at[c], new_weights.at[c], sems.at[0, c]) for c in range(final)]
    copies += [pltpu.make_async_copy(new_momentum_v.at[c], new_momentum.at[c], sems.at[1, c]) for c in range(CHUNKS)]
    for copy in copies:
        copy.start()
    last_v[...] = last_w[...] - new_weights_v[final]
    last_copy = pltpu.make_async_copy(last_v, new_weights.at[final], sems.at[0, final])
    last_copy.start()
    for copy in copies:
        copy.wait()
    last_copy.wait()


def exchange(slopes, moments, weights):
    shape = (CHUNKS, NZ, NP, 4, 256)
    whole = jax.ShapeDtypeStruct(shape, jnp.float32)
    split = pltpu.VMEM(shape, jnp.float32)
    plane = pltpu.VMEM((CHUNKS, NP, NZ, 4, 256), jnp.float32)
    chunk = jax.ShapeDtypeStruct(shape[1:], jnp.float32)
    new_weights, new_momentum, last = pl.pallas_call(
        kernel,
        name="exchange",
        out_shape=(whole, whole, chunk),
        in_specs=[pl.BlockSpec(memory_space=pltpu.HBM)] * 3,
        out_specs=[pl.BlockSpec(memory_space=pltpu.VMEM)] * 3,
        scratch_shapes=[split, split, pltpu.VMEM((CHUNKS - 1, *shape[1:]), jnp.float32), split, plane, plane, split, pltpu.VMEM((128, 1024), jnp.float32)]
        + [pltpu.VMEM((256, 1024), jnp.bfloat16), pltpu.VMEM((128, 1024), jnp.bfloat16)]
        + [pltpu.SemaphoreType.REGULAR((3,))]
        + [pltpu.SemaphoreType.DMA((CHUNKS,))] * 2
        + [pltpu.SemaphoreType.DMA((2,))]
        + [pltpu.SemaphoreType.DMA((CHUNKS,))] * 8,
        compiler_params=pltpu.CompilerParams(collective_id=0, has_side_effects=True, vmem_limit_bytes=40 * 2**20),
    )(*[pltpu.with_memory_space_constraint(a.reshape(shape), pltpu.HBM) for a in (slopes, moments, weights)])
    new_weights, new_momentum = pl.pallas_call(
        put_out,
        name="put_out",
        out_shape=(whole, whole),
        in_specs=[pl.BlockSpec(memory_space=pltpu.VMEM)] * 3,
        out_specs=[pl.BlockSpec(memory_space=pltpu.HBM)] * 2,
        scratch_shapes=[pltpu.VMEM(shape[1:], jnp.float32), pltpu.SemaphoreType.DMA((2, CHUNKS))],
        compiler_params=pltpu.CompilerParams(vmem_limit_bytes=8 * 2**20),
    )(new_weights, new_momentum, last)
    return new_weights.reshape(slopes.shape), new_momentum.reshape(slopes.shape)


def body(slopes_in, moments_in, weights_in):
    return exchange(slopes_in, moments_in, weights_in)


def solution(mesh):
    placed = (P("job", "fsdp", "tp"), P("job", "fsdp", "tp"), P("job", "fsdp", "tp"))
    return jax.shard_map(
        body,
        mesh=mesh,
        in_specs=placed,
        out_specs=(P("job", "fsdp", "tp"), P("job", "fsdp", "tp")),
        check_vma=False,
    )
```
